8 devices in a mesh: pod: 1 (over z), dp: 2 (over y), ep: 4 (over x, core).
Axes of the slice: x: 2, y: 2, z: 1, core: 2. Of those that a mesh axis runs over, the one named last changes fastest.
Arguments:
- x_start: bfloat16 [8192, 1024], P(('pod', 'dp', 'ep'))
- route_a: int32 [8192, 2], P(('pod', 'dp', 'ep'))
- route_b: int32 [8192, 2], P(('pod', 'dp', 'ep'))
- gate_a: float32 [8192, 2], P(('pod', 'dp', 'ep'))
- gate_b: float32 [8192, 2], P(('pod', 'dp', 'ep'))
- grad_out: bfloat16 [8192, 1024], P(('pod', 'dp', 'ep'))
- w1_a: bfloat16 [16, 1024, 1536], P('ep')
- w3_a: bfloat16 [16, 1024, 1536], P('ep')
- w2_a: bfloat16 [16, 1536, 1024], P('ep')
- w1_b: bfloat16 [16, 1024, 1536], P('ep')
- w3_b: bfloat16 [16, 1024, 1536], P('ep')
- w2_b: bfloat16 [16, 1536, 1024], P('ep')
Outputs:
- output 1: bfloat16 [8192, 1024], P(('pod', 'dp', 'ep'))
- output 2: bfloat16 [8192, 1024], P(('pod', 'dp', 'ep'))
- output 3: float32 [16, 1024, 1536], P(('pod', 'ep'), 'dp')
- output 4: float32 [16, 1024, 1536], P(('pod', 'ep'), 'dp')
- output 5: float32 [16, 1536, 1024], P(('pod', 'ep'), 'dp')
- output 6: float32 [16, 1024, 1536], P(('pod', 'ep'), 'dp')
- output 7: float32 [16, 1024, 1536], P(('pod', 'ep'), 'dp')
- output 8: float32 [16, 1536, 1024], P(('pod', 'ep'), 'dp')
- output 9: float32 [8192, 2], P(('pod', 'dp', 'ep'))
- output 10: float32 [8192, 2], P(('pod', 'dp', 'ep'))
All inputs are finite; a program needn't handle non-finite values.
Results may differ from the reference program's by a relative error of at most 0.0078204.
Values are sent between devices in bfloat16 or wider.
A program may use at most 1 GiB of HBM per device.

```python
import jax
import jax.numpy as jnp
from jax import lax

MODEL_DIM = 1024
FFN_DIM = 1536
EXPERTS = 16
TOP_K = 2
TOKENS_DEV = 1024
PART_DEVS = 8

CAPACITY = 3 * TOKENS_DEV * TOP_K // (2 * EXPERTS)
MEAN_LOAD = TOKENS_DEV * TOP_K // EXPERTS
PART_TOKENS = PART_DEVS * TOKENS_DEV
SLOT_ROWS = PART_DEVS * CAPACITY


def draw_routing(route_key):
    def one_device(dev_key):
        key_order, key_tokens = jax.random.split(dev_key)
        expert_order = jax.random.permutation(key_order, EXPERTS).astype(jnp.int32)
        counts = jnp.where(jnp.arange(EXPERTS) % 2 == 0, CAPACITY, 2 * MEAN_LOAD - CAPACITY)
        flat_ids = jnp.repeat(expert_order, counts, total_repeat_length=TOKENS_DEV * TOP_K)
        id_table = flat_ids.reshape(TOP_K, TOKENS_DEV).T
        return id_table[jax.random.permutation(key_tokens, TOKENS_DEV)]
    dev_keys = jax.random.split(route_key, PART_DEVS)
    return jax.vmap(one_device)(dev_keys).reshape(PART_TOKENS, TOP_K).astype(jnp.int32)


def setup_inputs(seed: int = 0, part: int = 0) -> dict:
    base_key = jax.random.key(seed)
    shared_key, group_key = jax.random.split(base_key)
    group_key = jax.random.fold_in(group_key, part)
    part_keys = jax.random.split(group_key, 6)
    weight_keys = jax.random.split(shared_key, 6)
    up_scale = MODEL_DIM ** -0.5
    down_scale = FFN_DIM ** -0.5
    gate_scale = TOP_K ** -0.5
    up_shape = (EXPERTS, MODEL_DIM, FFN_DIM)
    down_shape = (EXPERTS, FFN_DIM, MODEL_DIM)
    tok_shape = (PART_TOKENS, MODEL_DIM)
    pair_shape = (PART_TOKENS, TOP_K)

    def draw_weight(draw_key, arr_shape, std_scale):
        return (jax.random.normal(draw_key, arr_shape, jnp.float32) * std_scale).astype(jnp.bfloat16)

    return {
        'x_start': jax.random.normal(part_keys[0], tok_shape, jnp.float32).astype(jnp.bfloat16),
        'route_a': draw_routing(part_keys[1]),
        'route_b': draw_routing(part_keys[2]),
        'gate_a': jax.random.uniform(part_keys[3], pair_shape, jnp.float32, 0.5, 1.5) * gate_scale,
        'gate_b': jax.random.uniform(part_keys[4], pair_shape, jnp.float32, 0.5, 1.5) * gate_scale,
        'grad_out': jax.random.normal(part_keys[5], tok_shape, jnp.float32).astype(jnp.bfloat16),
        'w1_a': draw_weight(weight_keys[0], up_shape, up_scale),
        'w3_a': draw_weight(weight_keys[1], up_shape, up_scale),
        'w2_a': draw_weight(weight_keys[2], down_shape, down_scale),
        'w1_b': draw_weight(weight_keys[3], up_shape, up_scale),
        'w3_b': draw_weight(weight_keys[4], up_shape, up_scale),
        'w2_b': draw_weight(weight_keys[5], down_shape, down_scale),
    }


def pair_rows(route_ids):
    per_dev = route_ids.reshape(PART_DEVS, TOKENS_DEV * TOP_K)
    expert_range = jnp.arange(EXPERTS, dtype=jnp.int32)

    def dev_slots(dev_ids):
        onehot = (dev_ids[:, None] == expert_range[None, :]).astype(jnp.int32)
        earlier = jnp.cumsum(onehot, axis=0) - onehot
        return jnp.sum(earlier * onehot, axis=1)

    slot_ids = lax.map(dev_slots, per_dev)
    dev_index = jnp.arange(PART_DEVS, dtype=jnp.int32)[:, None]
    return (per_dev * SLOT_ROWS + dev_index * CAPACITY + slot_ids).reshape(-1)


def to_buffer(pair_vals, pair_row):
    filled = jnp.zeros((EXPERTS * SLOT_ROWS,) + pair_vals.shape[1:], pair_vals.dtype).at[pair_row].set(pair_vals)
    return filled.reshape((EXPERTS, SLOT_ROWS) + pair_vals.shape[1:])


def from_buffer(filled, pair_row):
    flat_rows = filled.reshape((EXPERTS * SLOT_ROWS,) + filled.shape[2:])
    picked = flat_rows[pair_row]
    return picked.reshape((PART_TOKENS, TOP_K) + filled.shape[2:])


def expert_fwd(operands):
    tok_rows, w_up1, w_up3, w_down = operands
    pre_one = jnp.dot(tok_rows, w_up1, preferred_element_type=jnp.float32)
    pre_three = jnp.dot(tok_rows, w_up3, preferred_element_type=jnp.float32)
    hidden = (jax.nn.silu(pre_one) * pre_three).astype(jnp.bfloat16)
    return jnp.dot(hidden, w_down, preferred_element_type=jnp.float32).astype(jnp.bfloat16)


def expert_bwd(operands):
    tok_rows, grad_rows, gate_rows, w_up1, w_up3, w_down = operands
    pre_one = jnp.dot(tok_rows, w_up1, preferred_element_type=jnp.float32)
    pre_three = jnp.dot(tok_rows, w_up3, preferred_element_type=jnp.float32)
    sig_one = jax.nn.sigmoid(pre_one)
    act_one = pre_one * sig_one
    hidden = (act_one * pre_three).astype(jnp.bfloat16)
    back_proj = jnp.dot(grad_rows, w_down.T, preferred_element_type=jnp.float32)
    gate_grad = jnp.sum(back_proj * hidden.astype(jnp.float32), axis=1)
    scaled_dy = (gate_rows[:, None] * grad_rows.astype(jnp.float32)).astype(jnp.bfloat16)
    dw_down = jnp.dot(hidden.T, scaled_dy, preferred_element_type=jnp.float32)
    d_hidden = gate_rows[:, None] * back_proj
    d_pre_one = (d_hidden * pre_three * sig_one * (1.0 + pre_one * (1.0 - sig_one))).astype(jnp.bfloat16)
    d_pre_three = (d_hidden * act_one).astype(jnp.bfloat16)
    dw_up1 = jnp.dot(tok_rows.T, d_pre_one, preferred_element_type=jnp.float32)
    dw_up3 = jnp.dot(tok_rows.T, d_pre_three, preferred_element_type=jnp.float32)
    grad_in = (jnp.dot(d_pre_one, w_up1.T, preferred_element_type=jnp.float32)
               + jnp.dot(d_pre_three, w_up3.T, preferred_element_type=jnp.float32)).astype(jnp.bfloat16)
    return grad_in, gate_grad, dw_up1, dw_up3, dw_down


def layer_fwd(x_in, pair_row, gate_vals, w_up1, w_up3, w_down):
    tok_rows = to_buffer(jnp.repeat(x_in, TOP_K, axis=0), pair_row)
    out_rows = lax.map(expert_fwd, (tok_rows, w_up1, w_up3, w_down))
    pair_out = from_buffer(out_rows, pair_row).astype(jnp.float32)
    mixed_sum = jnp.sum(gate_vals[:, :, None] * pair_out, axis=1)
    return (x_in.astype(jnp.float32) + mixed_sum).astype(jnp.bfloat16)


def layer_bwd(x_in, pair_row, gate_vals, w_up1, w_up3, w_down, grad_in):
    tok_rows = to_buffer(jnp.repeat(x_in, TOP_K, axis=0), pair_row)
    grad_rows = to_buffer(jnp.repeat(grad_in, TOP_K, axis=0), pair_row)
    gate_rows = to_buffer(gate_vals.reshape(-1), pair_row)
    du_rows, gate_grad, dw_up1, dw_up3, dw_down = lax.map(expert_bwd, (tok_rows, grad_rows, gate_rows, w_up1, w_up3, w_down))
    pair_grad = from_buffer(du_rows, pair_row).astype(jnp.float32)
    grad_x = (grad_in.astype(jnp.float32) + jnp.sum(pair_grad, axis=1)).astype(jnp.bfloat16)
    return grad_x, dw_up1, dw_up3, dw_down, from_buffer(gate_grad, pair_row)


def reference(x_start, route_a, route_b, gate_a, gate_b, grad_out, w1_a, w3_a, w2_a, w1_b, w3_b, w2_b):
    rows_a = pair_rows(route_a)
    rows_b = pair_rows(route_b)
    x_mid = layer_fwd(x_start, rows_a, gate_a, w1_a, w3_a, w2_a)
    x_final = layer_fwd(x_mid, rows_b, gate_b, w1_b, w3_b, w2_b)
    grad_mid, dw1_b, dw3_b, dw2_b, dgate_b = layer_bwd(x_mid, rows_b, gate_b, w1_b, w3_b, w2_b, grad_out)
    grad_x, dw1_a, dw3_a, dw2_a, dgate_a = layer_bwd(x_start, rows_a, gate_a, w1_a, w3_a, w2_a, grad_mid)
    return (x_final, grad_x, dw1_a, dw3_a, dw2_a, dw1_b, dw3_b, dw2_b, dgate_a, dgate_b)
```

```python
import functools

import jax
import jax.numpy as jnp
from jax import lax
from jax.experimental import pallas as pl
from jax.experimental.pallas import tpu as pltpu
from jax.sharding import PartitionSpec as P

F32 = jnp.float32
BF16 = jnp.bfloat16
NN = (((1,), (0,)), ((), ()))
NT = (((1,), (1,)), ((), ()))
TN = (((0,), (0,)), ((), ()))
VMEM_LIMIT = 60 * 1024 * 1024


def mm(lhs, rhs, dims=NN):
    return lax.dot_general(lhs, rhs, dims, preferred_element_type=F32)


def params():
    return pltpu.CompilerParams(vmem_limit_bytes=VMEM_LIMIT, dimension_semantics=('arbitrary',))


def cost(flops, nbytes):
    return pl.CostEstimate(flops=int(flops), bytes_accessed=int(nbytes), transcendentals=0)


def plan_kernel(capacity, in_ref, row_ref, col_ref):
    n_tok = in_ref.shape[0]
    lane = lax.broadcasted_iota(jnp.int32, (n_tok, 128), 1)
    earlier = (lax.broadcasted_iota(jnp.int32, (n_tok, n_tok), 0)
               > lax.broadcasted_iota(jnp.int32, (n_tok, n_tok), 1))
    lower = jnp.where(earlier, 1.0, 0.0).astype(BF16)
    table = jnp.zeros((n_tok, 128), F32)
    for layer in range(2):
        ids = [in_ref[:, 2 * layer + j:2 * layer + j + 1] for j in range(2)]
        hot = [jnp.where(lane == i.astype(jnp.int32), 1.0, 0.0) for i in ids]
        count = mm(lower, (hot[0] + hot[1]).astype(BF16))
        for j in range(2):
            row = ids[j] * float(capacity) + jnp.sum(count * hot[j], axis=1, keepdims=True)
            table = jnp.where(lane == 2 * layer + j, row, table)
            table = jnp.where(lane == 4 + 2 * layer + j, in_ref[:, 4 + 2 * layer + j:5 + 2 * layer + j], table)
    col_ref[...] = table
    row_ref[...] = jnp.transpose(table)[:8]


def make_plan(packed, capacity):
    n_tok = packed.shape[0]
    return pl.pallas_call(
        functools.partial(plan_kernel, capacity),
        out_shape=(jax.ShapeDtypeStruct((8, n_tok), F32), jax.ShapeDtypeStruct((n_tok, 128), F32)),
        compiler_params=pltpu.CompilerParams(vmem_limit_bytes=VMEM_LIMIT),
        cost_estimate=cost(4 * n_tok * n_tok * 128, 1 << 20), name='plan')(packed)


def pick_kernel(layer, with_gate, base_ref, plan_ref, tok_ref, out_ref, *gate_out):
    n_exp, _, cap, dim = out_ref.shape
    n_rows, n_tok = n_exp * cap, tok_ref.shape[1]
    send_row = base_ref[0] + lax.broadcasted_iota(jnp.int32, (n_rows, n_tok), 0)
    hits = [plan_ref[0, 2 * layer + j:2 * layer + j + 1, :].astype(jnp.int32) == send_row for j in range(2)]
    select = jnp.where(hits[0] | hits[1], 1.0, 0.0).astype(BF16)
    out_ref[:, 0] = mm(select, tok_ref[0]).astype(BF16).reshape(n_exp, cap, dim)
    if with_gate:
        gates = [plan_ref[0, 4 + 2 * layer + j:5 + 2 * layer + j, :] for j in range(2)]
        picked = jnp.sum(jnp.where(hits[0], gates[0], 0.0) + jnp.where(hits[1], gates[1], 0.0), axis=1, keepdims=True)
        gate_out[0][:, 0] = jnp.broadcast_to(picked, (n_rows, 128)).reshape(n_exp, cap, 128)


def pick_rows(tokens, plans, place, layer, n_exp, cap, with_gate=False):
    n_src, n_tok, dim = tokens.shape
    out_shape = [jax.ShapeDtypeStruct((n_exp, n_src, cap, dim), BF16)]
    out_specs = [pl.BlockSpec((n_exp, 1, cap, dim), lambda s, _: (0, s, 0, 0))]
    if with_gate:
        out_shape.append(jax.ShapeDtypeStruct((n_exp, n_src, cap, 128), F32))
        out_specs.append(pl.BlockSpec((n_exp, 1, cap, 128), lambda s, _: (0, s, 0, 0)))
    picked = pl.pallas_call(
        functools.partial(pick_kernel, layer, with_gate),
        out_shape=out_shape,
        grid_spec=pltpu.PrefetchScalarGridSpec(
            num_scalar_prefetch=1, grid=(n_src,),
            in_specs=[pl.BlockSpec((1, 8, n_tok), lambda s, _: (s, 0, 0)),
                      pl.BlockSpec((1, n_tok, dim), lambda s, _: (s, 0, 0))],
            out_specs=out_specs),
        compiler_params=params(),
        cost_estimate=cost(2 * n_src * n_exp * cap * n_tok * dim, tokens.size * 4), name='pick')(place, plans, tokens)
    return picked if with_gate else picked[0]


def ffn_kernel(chunk, _, x_ref, w1_ref, w3_ref, w2_ref, out_ref, hid_ref):
    rows = x_ref.shape[1] * x_ref.shape[2]
    x = x_ref[0].reshape(rows, x_ref.shape[3])

    def step(c, carry):
        cols = pl.ds(pl.multiple_of(c * chunk, chunk), chunk)
        pre_one = mm(x, w1_ref[0, :, cols])
        pre_three = mm(x, w3_ref[0, :, cols])
        hid_ref[:, cols] = (pre_one * jax.nn.sigmoid(pre_one) * pre_three).astype(BF16)
        return carry

    lax.fori_loop(0, hid_ref.shape[1] // chunk, step, 0)
    out = mm(hid_ref[...], w2_ref[0])
    out_ref[:, 0] = out.astype(BF16).reshape(out_ref.shape[0], out_ref.shape[2], out_ref.shape[3])


def ffn(rows_x, place, w1, w3, w2, n_grp, pick_group):
    n_exp, _, cap, dim = rows_x.shape
    hid = w1.shape[2]
    group = (lambda e, p: (e, p[1], 0, 0)) if pick_group else (lambda e, p: (e, 0, 0, 0))
    whole = lambda e, p: (e, 0, 0)
    n_rows = n_exp * n_grp * cap
    return pl.pallas_call(
        functools.partial(ffn_kernel, 512),
        out_shape=jax.ShapeDtypeStruct((n_grp, n_exp, cap, dim), BF16),
        grid_spec=pltpu.PrefetchScalarGridSpec(
            num_scalar_prefetch=1, grid=(n_exp,),
            in_specs=[pl.BlockSpec((1, n_grp, cap, dim), group),
                      pl.BlockSpec((1, dim, hid), whole), pl.BlockSpec((1, dim, hid), whole),
                      pl.BlockSpec((1, hid, dim), whole)],
            out_specs=pl.BlockSpec((n_grp, 1, cap, dim), lambda e, p: (0, e, 0, 0)),
            scratch_shapes=[pltpu.VMEM((n_grp * cap, hid), BF16)]),
        compiler_params=params(),
        cost_estimate=cost(6 * n_rows * dim * hid, 6 * n_exp * dim * hid + 4 * n_rows * dim),
        name='ffn')(place, rows_x, w1, w3, w2)


def act_kernel(chunk, own, _, x_ref, dy_ref, gate_ref, w1_ref, w3_ref, w2_ref, da1_ref, da3_ref, h_ref, *own_refs):
    n_grp, cap, dim = x_ref.shape[1:]
    rows = n_grp * cap
    hid = w1_ref.shape[2]
    x = x_ref[0].reshape(rows, dim)
    dy = dy_ref[0].reshape(rows, dim)
    gate = gate_ref[0].reshape(rows, 128)[:, :1]

    def step(c, gate_grad):
        cols = pl.ds(pl.multiple_of(c * chunk, chunk), chunk)
        pre_one = mm(x, w1_ref[0, :, cols])
        pre_three = mm(x, w3_ref[0, :, cols])
        back = mm(dy, w2_ref[0, cols, :], NT)
        sig = jax.nn.sigmoid(pre_one)
        act = pre_one * sig
        hidden = (act * pre_three).astype(BF16)
        d_hidden = gate * back
        d_one = d_hidden * pre_three * sig * (1.0 + pre_one * (1.0 - sig))
        h_ref[0, :, :, cols] = hidden.reshape(n_grp, cap, chunk)
        da1_ref[0, :, :, cols] = d_one.astype(BF16).reshape(n_grp, cap, chunk)
        da3_ref[0, :, :, cols] = (d_hidden * act).astype(BF16).reshape(n_grp, cap, chunk)
        if own:
            gate_grad = gate_grad + jnp.sum(hidden.astype(F32) * back, axis=1, keepdims=True)
        return gate_grad

    gate_grad = lax.fori_loop(0, hid // chunk, step, jnp.zeros((rows, 1), F32))
    if own:
        du_ref, dgate_ref = own_refs
        dgate_ref[:, 0] = jnp.broadcast_to(gate_grad, (rows, 128)).reshape(n_grp, cap, 128)
        du = mm(da1_ref[0].reshape(rows, hid), w1_ref[0], NT) + mm(da3_ref[0].reshape(rows, hid), w3_ref[0], NT)
        du_ref[:, 0] = du.astype(BF16).reshape(n_grp, cap, dim)


def act(rows_x, rows_dy, gates, place, w1, w3, w2, n_grp, own):
    n_exp, _, cap, dim = rows_x.shape
    hid = w1.shape[2]
    group = (lambda e, p: (e, p[1], 0, 0)) if own else (lambda e, p: (e, 1 - p[1], 0, 0))
    whole = lambda e, p: (e, 0, 0)
    mine = lambda e, p: (e, 0, 0, 0)
    back = lambda e, p: (0, e, 0, 0)
    out_shape = [jax.ShapeDtypeStruct((n_exp, n_grp, cap, hid), BF16)] * 3
    out_specs = [pl.BlockSpec((1, n_grp, cap, hid), mine)] * 3
    if own:
        out_shape += [jax.ShapeDtypeStruct((n_grp, n_exp, cap, dim), BF16),
                      jax.ShapeDtypeStruct((n_grp, n_exp, cap, 128), F32)]
        out_specs += [pl.BlockSpec((n_grp, 1, cap, dim), back), pl.BlockSpec((n_grp, 1, cap, 128), back)]
    n_rows = n_exp * n_grp * cap
    return pl.pallas_call(
        functools.partial(act_kernel, 512, own),
        out_shape=out_shape,
        grid_spec=pltpu.PrefetchScalarGridSpec(
            num_scalar_prefetch=1, grid=(n_exp,),
            in_specs=[pl.BlockSpec((1, n_grp, cap, dim), group), pl.BlockSpec((1, n_grp, cap, dim), group),
                      pl.BlockSpec((1, n_grp, cap, 128), group),
                      pl.BlockSpec((1, dim, hid), whole), pl.BlockSpec((1, dim, hid), whole),
                      pl.BlockSpec((1, hid, dim), whole)],
            out_specs=out_specs),
        compiler_params=params(),
        cost_estimate=cost((10 if own else 6) * n_rows * dim * hid, 6 * n_exp * dim * hid + 8 * n_rows * hid),
        name='act_own' if own else 'act_other')(place, rows_x, rows_dy, gates, w1, w3, w2)


def dw_kernel(_, xs_ref, xo_ref, dys_ref, dyo_ref, gs_ref, go_ref, a1s_ref, a1o_ref, a3s_ref, a3o_ref, hs_ref, ho_ref,
              dw1_ref, dw3_ref, dw2_ref):
    def flat(ref):
        return ref[0].reshape(ref.shape[1] * ref.shape[2], ref.shape[3])

    xs, xo = flat(xs_ref), flat(xo_ref)
    dw1_ref[0] = mm(xs, flat(a1s_ref), TN) + mm(xo, flat(a1o_ref), TN)
    dw3_ref[0] = mm(xs, flat(a3s_ref), TN) + mm(xo, flat(a3o_ref), TN)
    gdy_s = (flat(gs_ref)[:, :1] * flat(dys_ref).astype(F32)).astype(BF16)
    gdy_o = (flat(go_ref)[:, :1] * flat(dyo_ref).astype(F32)).astype(BF16)
    dw2_ref[0] = mm(flat(hs_ref), gdy_s, TN) + mm(flat(ho_ref), gdy_o, TN)


def dweights(rows_x, rows_dy, gates, place, acts_own, acts_other, n_grp, n_dp):
    n_exp, _, cap, dim = rows_x.shape
    hid = acts_own[0].shape[3]
    dim_part, hid_part = dim // n_dp, hid // n_dp
    x_spec = [pl.BlockSpec((1, n_grp, cap, dim_part), lambda e, p: (e, p[1], 0, p[1])),
              pl.BlockSpec((1, n_grp, cap, dim_part), lambda e, p: (e, 1 - p[1], 0, p[1]))]
    both = lambda width: [pl.BlockSpec((1, n_grp, cap, width), lambda e, p: (e, p[1], 0, 0)),
                          pl.BlockSpec((1, n_grp, cap, width), lambda e, p: (e, 1 - p[1], 0, 0))]
    a_spec = pl.BlockSpec((1, n_grp, cap, hid), lambda e, p: (e, 0, 0, 0))
    h_spec = pl.BlockSpec((1, n_grp, cap, hid_part), lambda e, p: (e, 0, 0, p[1]))
    n_rows = n_exp * n_grp * cap
    up = jax.ShapeDtypeStruct((n_exp, dim_part, hid), F32)
    down = jax.ShapeDtypeStruct((n_exp, hid_part, dim), F32)
    whole = lambda e, p: (e, 0, 0)
    (a1s, a3s, hs), (a1o, a3o, ho) = acts_own, acts_other
    return pl.pallas_call(
        dw_kernel,
        out_shape=[up, up, down],
        grid_spec=pltpu.PrefetchScalarGridSpec(
            num_scalar_prefetch=1, grid=(n_exp,),
            in_specs=x_spec + both(dim) + both(128) + [a_spec] * 4 + [h_spec] * 2,
            out_specs=[pl.BlockSpec((1, dim_part, hid), whole)] * 2 + [pl.BlockSpec((1, hid_part, dim), whole)]),
        compiler_params=params(),
        cost_estimate=cost(6 * n_rows * dim * hid, 10 * n_rows * hid + 6 * n_exp * dim * hid),
        name='dweights')(place, rows_x, rows_x, rows_dy, rows_dy, gates, gates, a1s, a1o, a3s, a3o, hs, ho)


def hot_rows(plan_ref, col, n_rows):
    row = lax.broadcasted_iota(jnp.int32, (plan_ref.shape[0], n_rows), 1)
    return plan_ref[:, col:col + 1].astype(jnp.int32) == row


def mix_kernel(layer, x_ref, plan_ref, rows_ref, out_ref):
    total = None
    for j in range(2):
        hit = jnp.where(hot_rows(plan_ref, 2 * layer + j, rows_ref.shape[0]), 1.0, 0.0).astype(BF16)
        gate = plan_ref[:, 4 + 2 * layer + j:5 + 2 * layer + j]
        term = gate * mm(hit, rows_ref[...])
        total = term if total is None else total + term
    out_ref[...] = (x_ref[...].astype(F32) + total).astype(BF16)


def add_kernel(layer, dy_ref, plan_ref, rows_ref, dgate_ref, out_ref, gate_ref):
    n_rows = rows_ref.shape[0]
    hits = [hot_rows(plan_ref, 2 * layer + j, n_rows) for j in range(2)]
    hit = jnp.where(hits[0] | hits[1], 1.0, 0.0).astype(BF16)
    out_ref[...] = (dy_ref[...].astype(F32) + mm(hit, rows_ref[...])).astype(BF16)
    lane = lax.broadcasted_iota(jnp.int32, gate_ref.shape, 1)
    grads = [jnp.sum(jnp.where(h, dgate_ref[0:1, :], 0.0), axis=1, keepdims=True) for h in hits]
    gate_ref[...] = jnp.where(lane == 0, grads[0], jnp.where(lane == 1, grads[1], 0.0))


def combine(layer, x_in, plan_col, rows, dgate_rows=None):
    n_tok, dim = x_in.shape
    n_rows = rows.shape[0]
    tile = 256
    specs = [pl.BlockSpec((tile, dim), lambda t: (t, 0)), pl.BlockSpec((tile, 128), lambda t: (t, 0)),
             pl.BlockSpec((n_rows, dim), lambda t: (0, 0))]
    out = jax.ShapeDtypeStruct((n_tok, dim), BF16)
    est = cost(4 * n_tok * n_rows * dim, 2 * n_rows * dim)
    if dgate_rows is None:
        return pl.pallas_call(
            functools.partial(mix_kernel, layer), out_shape=out, grid=(n_tok // tile,),
            in_specs=specs, out_specs=specs[0], compiler_params=params(), cost_estimate=est,
            name='mix')(x_in, plan_col, rows)
    grad_x, dgate = pl.pallas_call(
        functools.partial(add_kernel, layer),
        out_shape=(out, jax.ShapeDtypeStruct((n_tok, 128), F32)), grid=(n_tok // tile,),
        in_specs=specs + [pl.BlockSpec((1, n_rows), lambda t: (0, 0))],
        out_specs=(specs[0], specs[1]), compiler_params=params(), cost_estimate=est,
        name='add_back')(x_in, plan_col, rows, dgate_rows)
    return grad_x, dgate[:, :2]


def solution(mesh):
    n_ep, n_dp = mesh.shape['ep'], mesh.shape['dp']
    tok_spec = P(('pod', 'dp', 'ep'), None)
    weight_spec = P('ep', None, None)
    grad_spec = P(('pod', 'ep'), 'dp', None)

    def local_step(x_start, route_a, route_b, gate_a, gate_b, grad_out, w1_a, w3_a, w2_a, w1_b, w3_b, w2_b):
        n_tok, dim = x_start.shape
        top_k = route_a.shape[1]
        n_local = w1_a.shape[0]
        n_experts = n_local * n_ep
        cap = 3 * n_tok * top_k // (2 * n_experts)
        ep_i, dp_i = lax.axis_index('ep'), lax.axis_index('dp')
        place = jnp.stack([ep_i * (n_local * cap), dp_i]).astype(jnp.int32)

        packed = jnp.concatenate([route_a.astype(F32), route_b.astype(F32), gate_a, gate_b], axis=1)
        plan_row, plan_col = make_plan(packed, cap)
        plans = lax.all_gather(plan_row, ('dp', 'ep'))
        plans_own = lax.dynamic_slice_in_dim(plans, dp_i * n_ep, n_ep, 0)

        def give_back(rows):
            returned = lax.all_to_all(rows, 'ep', 0, 0)
            return returned.reshape((n_experts * cap,) + rows.shape[3:])

        def experts_own(layer, rows_x, grads, weights):
            rows_dy, gates = pick_rows(grads, plans, place, layer, n_local, cap, with_gate=True)
            return rows_dy, gates, act(rows_x, rows_dy, gates, place, *weights, n_ep, True)

        def finish(layer, rows_x, grad_in, weights, rows_dy, gates, acts):
            da1, da3, h, du, dgate = acts
            other = act(rows_x, rows_dy, gates, place, *weights, n_ep, False)
            back = (give_back(du), give_back(dgate[..., 0]))
            dws = lambda acts_other: dweights(rows_x, rows_dy, gates, place, (da1, da3, h), acts_other, n_ep, n_dp)
            if layer == 0:
                (du_back, dgate_back), sums = hold((back, tuple(dws(other))))
            else:
                (du_back, dgate_back), other = hold((back, tuple(other)))
                sums = dws(other)
            grad_x, dgate_tok = combine(layer, grad_in, plan_col, du_back, dgate_back.reshape(1, -1))
            return grad_x, dgate_tok, sums

        hold = lax.optimization_barrier
        every = ('dp', 'ep')
        weights_a, weights_b = (w1_a, w3_a, w2_a), (w1_b, w3_b, w2_b)
        rows_a = pick_rows(lax.all_gather(x_start, 'ep'), plans_own, place, 0, n_local, cap)
        out_a = ffn(rows_a, place, *weights_a, n_ep, False)
        x_mid = combine(0, x_start, plan_col, give_back(out_a))
        x_kept, grad_kept, x_mid = hold((x_start, grad_out, x_mid))
        rows_b = pick_rows(lax.all_gather(x_mid, every), plans, place, 1, n_local, cap)
        out_b = ffn(rows_b, place, *weights_b, n_ep, True)
        grads_b, out_b = hold((lax.all_gather(grad_kept, every), out_b))
        own_b = experts_own(1, rows_b, grads_b, weights_b)
        grad_mid, dgate_b, dws_b = finish(1, rows_b, grad_kept, weights_b, *own_b)
        rows_a_again = pick_rows(lax.all_gather(x_kept, every), plans, place, 0, n_local, cap)
        grads_a, dws_b, out_b = hold((lax.all_gather(grad_mid, every), tuple(dws_b), out_b))
        rows_dy, gates, acts_a = experts_own(0, rows_a_again, grads_a, weights_a)
        acts_a, back_b = hold((tuple(acts_a), give_back(out_b)))
        grad_x, dgate_a, dws_a = finish(0, rows_a_again, grad_mid, weights_a, rows_dy, gates, acts_a)
        x_final = combine(1, x_mid, plan_col, back_b)
        (dw1_b, dw3_b, dw2_b), (dw1_a, dw3_a, dw2_a) = dws_b, dws_a
        return (x_final, grad_x, dw1_a, dw3_a, dw2_a, dw1_b, dw3_b, dw2_b, dgate_a, dgate_b)

    return jax.shard_map(local_step, mesh=mesh,
                         in_specs=(tok_spec,) * 6 + (weight_spec,) * 6,
                         out_specs=(tok_spec, tok_spec) + (grad_spec,) * 6 + (tok_spec, tok_spec),
                         check_vma=False)
```

```python
import functools

import jax
import jax.numpy as jnp
from jax import lax
from jax.experimental import pallas as pl
from jax.experimental.pallas import tpu as pltpu
from jax.sharding import PartitionSpec as P


F32 = jnp.float32
BF16 = jnp.bfloat16
NN = (((1,), (0,)), ((), ()))
NT = (((1,), (1,)), ((), ()))
TN = (((0,), (0,)), ((), ()))
VMEM_LIMIT = 60 * 1024 * 1024


def mm(lhs, rhs, dims=NN):
    return lax.dot_general(lhs, rhs, dims, preferred_element_type=F32)


def params(n_axes=1):
    return pltpu.CompilerParams(vmem_limit_bytes=VMEM_LIMIT, dimension_semantics=('arbitrary',) * n_axes)


def cost(flops, nbytes):
    return pl.CostEstimate(flops=int(flops), bytes_accessed=int(nbytes), transcendentals=0)


def plan_kernel(capacity, in_ref, row_ref, col_ref):
    n_tok = in_ref.shape[0]
    lane = lax.broadcasted_iota(jnp.int32, (n_tok, 128), 1)
    earlier = (lax.broadcasted_iota(jnp.int32, (n_tok, n_tok), 0)
               > lax.broadcasted_iota(jnp.int32, (n_tok, n_tok), 1))
    lower = jnp.where(earlier, 1.0, 0.0).astype(BF16)
    table = jnp.zeros((n_tok, 128), F32)
    for layer in range(2):
        ids = [in_ref[:, 2 * layer + j:2 * layer + j + 1] for j in range(2)]
        hot = [jnp.where(lane == i.astype(jnp.int32), 1.0, 0.0) for i in ids]
        count = mm(lower, (hot[0] + hot[1]).astype(BF16))
        for j in range(2):
            row = ids[j] * float(capacity) + jnp.sum(count * hot[j], axis=1, keepdims=True)
            table = jnp.where(lane == 2 * layer + j, row, table)
            table = jnp.where(lane == 4 + 2 * layer + j, in_ref[:, 4 + 2 * layer + j:5 + 2 * layer + j], table)
    col_ref[...] = table
    row_ref[...] = jnp.transpose(table)[:8]


def make_plan(packed, capacity):
    n_tok = packed.shape[0]
    return pl.pallas_call(
        functools.partial(plan_kernel, capacity),
        out_shape=(jax.ShapeDtypeStruct((8, n_tok), F32), jax.ShapeDtypeStruct((n_tok, 128), F32)),
        compiler_params=pltpu.CompilerParams(vmem_limit_bytes=VMEM_LIMIT),
        cost_estimate=cost(4 * n_tok * n_tok * 128, 1 << 20), name='plan')(packed)


def pick_into(layer, base_ref, plan_ref, tokens, out_ref, gate_refs):
    n_exp, _, cap, dim = out_ref.shape
    n_rows, n_tok = n_exp * cap, tokens.shape[0]
    send_row = base_ref[0] + lax.broadcasted_iota(jnp.int32, (n_rows, n_tok), 0)
    hits = [plan_ref[0, 2 * layer + j:2 * layer + j + 1, :].astype(jnp.int32) == send_row for j in range(2)]
    select = jnp.where(hits[0] | hits[1], 1.0, 0.0).astype(BF16)
    out_ref[:, 0] = mm(select, tokens).astype(BF16).reshape(n_exp, cap, dim)
    for gate_ref in gate_refs:
        gates = [plan_ref[0, 4 + 2 * layer + j:5 + 2 * layer + j, :] for j in range(2)]
        picked = jnp.sum(jnp.where(hits[0], gates[0], 0.0) + jnp.where(hits[1], gates[1], 0.0), axis=1, keepdims=True)
        gate_ref[:, 0] = jnp.broadcast_to(picked, (n_rows, 128)).reshape(n_exp, cap, 128)


def pick_kernel(layer, base_ref, plan_ref, tok_ref, out_ref, *gate_refs):
    pick_into(layer, base_ref, plan_ref, tok_ref[0], out_ref, gate_refs)


def pick_parts_kernel(layer, n_src, base_ref, plan_ref, *refs):
    tabs, (held, sem) = refs[:n_src], refs[-2:]
    out_ref, gate_refs = refs[n_src], refs[n_src + 1:-2]
    src = pl.program_id(0)

    def load(i):
        return pltpu.make_async_copy(tabs[i], held.at[i % 2], sem.at[i % 2])

    for i in range(n_src):
        @pl.when(src == i)
        def _():
            if i == 0:
                load(0).start()
            if i + 1 < n_src:
                load(i + 1).start()
            load(i).wait()

    pick_into(layer, base_ref, plan_ref, held[src % 2], out_ref, gate_refs)


def pick_rows(tokens, plans, place, layer, n_exp, cap, with_gate=False):
    split = isinstance(tokens, tuple)
    n_src = len(tokens) if split else tokens.shape[0]
    source = 2 + (n_src if split else 0)
    n_tok, dim = tokens[0].shape
    out_shape = [jax.ShapeDtypeStruct((n_exp, n_src, cap, dim), BF16)]
    out_specs = [pl.BlockSpec((n_exp, 1, cap, dim), lambda s, _: (0, s, 0, 0))]
    if with_gate:
        out_shape.append(jax.ShapeDtypeStruct((n_exp, n_src, cap, 128), F32))
        out_specs.append(pl.BlockSpec((n_exp, 1, cap, 128), lambda s, _: (0, s, 0, 0)))
    if split:
        kernel = functools.partial(pick_parts_kernel, layer, n_src)
        tok_specs = [pl.BlockSpec(memory_space=pltpu.HBM)] * n_src
        scratch = [pltpu.VMEM((2, n_tok, dim), BF16), pltpu.SemaphoreType.DMA((2,))]
    else:
        kernel = functools.partial(pick_kernel, layer)
        tok_specs = [pl.BlockSpec((1, n_tok, dim), lambda s, _: (s, 0, 0))]
        scratch = []
        tokens = (tokens,)
    picked = pl.pallas_call(
        kernel, out_shape=out_shape,
        grid_spec=pltpu.PrefetchScalarGridSpec(
            num_scalar_prefetch=1, grid=(n_src,),
            in_specs=[pl.BlockSpec((1, 8, n_tok), lambda s, p: (p[source + s], 0, 0))] + tok_specs,
            out_specs=out_specs, scratch_shapes=scratch),
        compiler_params=params(),
        cost_estimate=cost(2 * n_src * n_exp * cap * n_tok * dim, n_src * n_tok * dim * 4),
        name='pick_other' if split else 'pick')(place, plans, *tokens)
    return picked if with_gate else picked[0]


def flat(ref):
    return ref[0].reshape(ref.shape[1] * ref.shape[2], ref.shape[3])


def ffn_kernel(n_chunk, x_ref, w1_ref, w3_ref, w2_ref, out_ref, hid_ref):
    c = pl.program_id(1)
    x = flat(x_ref)
    chunk = w1_ref.shape[2]
    pre_one = mm(x, w1_ref[0])
    pre_three = mm(x, w3_ref[0])
    hid_ref[:, pl.ds(pl.multiple_of(c * chunk, chunk), chunk)] = (
        pre_one * jax.nn.sigmoid(pre_one) * pre_three).astype(BF16)

    @pl.when(c == n_chunk - 1)
    def _():
        out = mm(hid_ref[...], w2_ref[0])
        out_ref[:, 0] = out.astype(BF16).reshape(out_ref.shape[0], out_ref.shape[2], out_ref.shape[3])


def ffn(rows_x, w1, w3, w2, first, n_exp, chunk=512):
    _, n_grp, cap, dim = rows_x.shape
    hid = w1.shape[2]
    n_rows = n_exp * n_grp * cap
    up = pl.BlockSpec((1, dim, chunk), lambda e, c: (e + first, 0, c))
    return pl.pallas_call(
        functools.partial(ffn_kernel, hid // chunk),
        out_shape=jax.ShapeDtypeStruct((n_grp, n_exp, cap, dim), BF16),
        grid=(n_exp, hid // chunk),
        in_specs=[pl.BlockSpec((1, n_grp, cap, dim), lambda e, c: (e + first, 0, 0, 0)), up, up,
                  pl.BlockSpec((1, hid, dim), lambda e, c: (e + first, 0, 0))],
        out_specs=pl.BlockSpec((n_grp, 1, cap, dim), lambda e, c: (0, e, 0, 0)),
        scratch_shapes=[pltpu.VMEM((n_grp * cap, hid), BF16)],
        compiler_params=params(2),
        cost_estimate=cost(6 * n_rows * dim * hid, 6 * n_exp * dim * hid + 4 * n_rows * dim),
        name='ffn')(rows_x, w1, w3, w2)


def act_kernel(n_chunk, own, n_kept, x_ref, dy_ref, gate_ref, w1_ref, w3_ref, w2_ref, *refs):
    da1_ref, da3_ref, h_ref, *own_refs = refs[n_kept:]
    n_grp, cap, dim = x_ref.shape[1:]
    rows = n_grp * cap
    chunk = w1_ref.shape[2]
    c = pl.program_id(1)
    x, dy = flat(x_ref), flat(dy_ref)
    pre_one = mm(x, w1_ref[0])
    pre_three = mm(x, w3_ref[0])
    back = mm(dy, w2_ref[0], NT)
    sig = jax.nn.sigmoid(pre_one)
    act_one = pre_one * sig
    hidden = (act_one * pre_three).astype(BF16)
    d_hidden = flat(gate_ref)[:, :1] * back
    d_one = (d_hidden * pre_three * sig * (1.0 + pre_one * (1.0 - sig))).astype(BF16)
    d_three = (d_hidden * act_one).astype(BF16)
    h_ref[0] = hidden.reshape(n_grp, cap, chunk)
    da1_ref[0] = d_one.reshape(n_grp, cap, chunk)
    da3_ref[0] = d_three.reshape(n_grp, cap, chunk)
    if own:
        du_ref, dgate_ref, total_ref = own_refs

        @pl.when(c == 0)
        def _():
            total_ref[...] = jnp.zeros_like(total_ref)
            dgate_ref[...] = jnp.zeros_like(dgate_ref)

        gate_grad = jnp.sum(hidden.astype(F32) * back, axis=1, keepdims=True)
        dgate_ref[:, 0] += jnp.broadcast_to(gate_grad, (rows, 128)).reshape(n_grp, cap, 128)
        total_ref[...] += mm(d_one, w1_ref[0], NT) + mm(d_three, w3_ref[0], NT)

        @pl.when(c == n_chunk - 1)
        def _():
            du_ref[:, 0] = total_ref[...].astype(BF16).reshape(n_grp, cap, dim)


def act(rows_x, rows_dy, gates, w1, w3, w2, first, n_exp, own, kept=(), chunk=512):
    n_all, n_grp, cap, dim = rows_x.shape
    hid = w1.shape[2]
    n_rows = n_exp * n_grp * cap
    rows = lambda e, c: (e + first, 0, 0, 0)
    back = lambda e, c: (0, e, 0, 0)
    up = pl.BlockSpec((1, dim, chunk), lambda e, c: (e + first, 0, c))
    out_shape = [jax.ShapeDtypeStruct((n_all, n_grp, cap, hid), BF16)] * 3
    out_specs = [pl.BlockSpec((1, n_grp, cap, chunk), lambda e, c: (e + first, 0, 0, c))] * 3
    scratch = []
    if own:
        out_shape += [jax.ShapeDtypeStruct((n_grp, n_exp, cap, dim), BF16),
                      jax.ShapeDtypeStruct((n_grp, n_exp, cap, 128), F32)]
        out_specs += [pl.BlockSpec((n_grp, 1, cap, dim), back), pl.BlockSpec((n_grp, 1, cap, 128), back)]
        scratch = [pltpu.VMEM((n_grp * cap, dim), F32)]
    return pl.pallas_call(
        functools.partial(act_kernel, hid // chunk, own, len(kept)),
        out_shape=out_shape, grid=(n_exp, hid // chunk),
        in_specs=[pl.BlockSpec((1, n_grp, cap, dim), rows), pl.BlockSpec((1, n_grp, cap, dim), rows),
                  pl.BlockSpec((1, n_grp, cap, 128), rows), up, up,
                  pl.BlockSpec((1, chunk, dim), lambda e, c: (e + first, c, 0))]
        + [pl.BlockSpec(memory_space=pltpu.HBM)] * len(kept),
        out_specs=out_specs, scratch_shapes=scratch, compiler_params=params(2),
        input_output_aliases={6 + i: i for i in range(len(kept))},
        cost_estimate=cost((10 if own else 6) * n_rows * dim * hid, 6 * n_exp * dim * hid + 8 * n_rows * hid),
        name='act_own' if own else 'act_other')(rows_x, rows_dy, gates, w1, w3, w2, *kept)


def dw_kernel(_, xs_ref, xo_ref, dys_ref, dyo_ref, gs_ref, go_ref, a1s_ref, a1o_ref, a3s_ref, a3o_ref, hs_ref, ho_ref,
              dw1_ref, dw3_ref, dw2_ref, gdy_s_ref, gdy_o_ref):
    @pl.when(pl.program_id(1) == 0)
    def _():
        gdy_s_ref[...] = (flat(gs_ref)[:, :1] * flat(dys_ref).astype(F32)).astype(BF16)
        gdy_o_ref[...] = (flat(go_ref)[:, :1] * flat(dyo_ref).astype(F32)).astype(BF16)

    xs, xo = flat(xs_ref), flat(xo_ref)
    dw1_ref[0] = mm(xs, flat(a1s_ref), TN) + mm(xo, flat(a1o_ref), TN)
    dw3_ref[0] = mm(xs, flat(a3s_ref), TN) + mm(xo, flat(a3o_ref), TN)
    dw2_ref[0] = mm(flat(hs_ref), gdy_s_ref[...], TN) + mm(flat(ho_ref), gdy_o_ref[...], TN)


def dweights(own, other, place, n_dp, n_chunk=3):
    (xs, dys, gs, a1s, a3s, hs), (xo, dyo, go, a1o, a3o, ho) = own, other
    n_exp, n_grp, cap, dim = xs.shape
    hid = a1s.shape[3]
    dim_part, hid_part = dim // n_dp, hid // n_dp
    up_c, down_c = hid // n_chunk, hid_part // n_chunk
    n_rows = n_exp * n_grp * cap
    x_spec = pl.BlockSpec((1, n_grp, cap, dim_part), lambda e, c, p: (e, 0, 0, p[1]))
    rows = lambda width: pl.BlockSpec((1, n_grp, cap, width), lambda e, c, p: (e, 0, 0, 0))
    a_spec = pl.BlockSpec((1, n_grp, cap, up_c), lambda e, c, p: (e, 0, 0, c))
    h_spec = pl.BlockSpec((1, n_grp, cap, down_c), lambda e, c, p: (e, 0, 0, n_chunk * p[1] + c))
    up = jax.ShapeDtypeStruct((n_exp, dim_part, hid), F32)
    down = jax.ShapeDtypeStruct((n_exp, hid_part, dim), F32)
    return pl.pallas_call(
        dw_kernel,
        out_shape=[up, up, down],
        grid_spec=pltpu.PrefetchScalarGridSpec(
            num_scalar_prefetch=1, grid=(n_exp, n_chunk),
            in_specs=[x_spec] * 2 + [rows(dim)] * 2 + [rows(128)] * 2 + [a_spec] * 4 + [h_spec] * 2,
            out_specs=[pl.BlockSpec((1, dim_part, up_c), lambda e, c, p: (e, 0, c))] * 2
            + [pl.BlockSpec((1, down_c, dim), lambda e, c, p: (e, c, 0))],
            scratch_shapes=[pltpu.VMEM((n_grp * cap, dim), BF16)] * 2),
        compiler_params=params(2),
        cost_estimate=cost(6 * n_rows * dim * hid, 10 * n_rows * hid + 6 * n_exp * dim * hid),
        name='dweights')(place, xs, xo, dys, dyo, gs, go, a1s, a1o, a3s, a3o, hs, ho)


def hits_of(plan_ref, layer, n_rows, n_ep, part, n_part):
    row = lax.broadcasted_iota(jnp.int32, (1, n_rows), 1)
    if n_part > 1:
        run = n_rows // n_ep
        owner = sum((row >= run * i).astype(jnp.int32) for i in range(1, n_ep))
        row = row + (owner * (n_part - 1) + part) * run
    return [plan_ref[:, 2 * layer + j:2 * layer + j + 1].astype(jnp.int32) == row for j in range(2)]


def one_hot(hit):
    return jnp.where(hit, 1.0, 0.0).astype(BF16)


def mix_kernel(layer, n_ep, part, n_part, base_ref, plan_ref, rows_ref, out_ref, partial_ref=None):
    hits = hits_of(plan_ref, layer, rows_ref.shape[0], n_ep, part, n_part)
    total = None
    for j in range(2):
        term = plan_ref[:, 4 + 2 * layer + j:5 + 2 * layer + j] * mm(one_hot(hits[j]), rows_ref[...])
        total = term if total is None else total + term
    finish(total, base_ref, out_ref, partial_ref)


def add_kernel(layer, n_ep, part, n_part, base_ref, plan_ref, rows_ref, out_ref, partial_ref=None):
    hits = hits_of(plan_ref, layer, rows_ref.shape[0], n_ep, part, n_part)
    finish(mm(one_hot(hits[0] | hits[1]), rows_ref[...]), base_ref, out_ref, partial_ref)


def finish(total, base_ref, out_ref, partial_ref):
    if partial_ref is not None:
        total = partial_ref[...] + total
    if base_ref is None:
        out_ref[...] = total
    else:
        out_ref[...] = (base_ref[...].astype(F32) + total).astype(BF16)


def combine(kernel, layer, x_in, plan_col, parts, n_ep, tile=256):
    n_tok, dim = x_in.shape
    wide = pl.BlockSpec((tile, dim), lambda t: (t, 0))
    partial = None
    for part, rows in enumerate(parts):
        n_rows = rows.shape[0]
        last = part == len(parts) - 1
        args = [plan_col, rows]
        specs = [pl.BlockSpec((tile, 128), lambda t: (t, 0)), pl.BlockSpec((n_rows, dim), lambda t: (0, 0))]
        if last:
            args, specs = [x_in] + args, [wide] + specs
        if partial is not None:
            args, specs = args + [partial], specs + [wide]

        def body(*refs, last=last, part=part, have=partial is not None):
            refs = list(refs)
            base = refs.pop(0) if last else None
            plan_ref, rows_ref = refs[0], refs[1]
            kernel(layer, n_ep, part, len(parts), base, plan_ref, rows_ref, refs[-1], refs[2] if have else None)

        partial = pl.pallas_call(
            body, out_shape=jax.ShapeDtypeStruct((n_tok, dim), BF16 if last else F32), grid=(n_tok // tile,),
            in_specs=specs, out_specs=wide, compiler_params=params(1),
            cost_estimate=cost((4 if kernel is mix_kernel else 2) * n_tok * n_rows * dim, 2 * n_rows * dim),
            name='mix' if kernel is mix_kernel else 'add_back')(*args)
    return partial


def gate_kernel(layer, plan_ref, dgate_ref, out_ref):
    lane = lax.broadcasted_iota(jnp.int32, out_ref.shape, 1)
    hits = hits_of(plan_ref, layer, dgate_ref.shape[1], 1, 0, 1)
    grads = [jnp.sum(jnp.where(h, dgate_ref[...], 0.0), axis=1, keepdims=True) for h in hits]
    out_ref[...] = jnp.where(lane == 0, grads[0], jnp.where(lane == 1, grads[1], 0.0))


def gate_back(layer, plan_col, dgate_rows, tile=256):
    n_tok = plan_col.shape[0]
    spec = pl.BlockSpec((tile, 128), lambda t: (t, 0))
    return pl.pallas_call(
        functools.partial(gate_kernel, layer), out_shape=jax.ShapeDtypeStruct((n_tok, 128), F32),
        grid=(n_tok // tile,), in_specs=[spec, pl.BlockSpec(dgate_rows.shape, lambda t: (0, 0))],
        out_specs=spec, compiler_params=params(1), cost_estimate=cost(5e9, 1 << 20),
        name='gate_back')(plan_col, dgate_rows)[:, :2]


def solution(mesh):
    n_ep, n_dp = mesh.shape['ep'], mesh.shape['dp']
    tok_spec = P(('pod', 'dp', 'ep'), None)
    weight_spec = P('ep', None, None)
    grad_spec = P(('pod', 'ep'), 'dp', None)
    hold = lax.optimization_barrier
    swap_dp = [(0, 1), (1, 0)]
    swap_core = [(i, i ^ 1) for i in range(n_ep)]

    def local_step(x_start, route_a, route_b, gate_a, gate_b, grad_out, w1_a, w3_a, w2_a, w1_b, w3_b, w2_b):
        n_tok, _ = x_start.shape
        top_k = route_a.shape[1]
        n_local = w1_a.shape[0]
        n_experts = n_local * n_ep
        cap = 3 * n_tok * top_k // (2 * n_experts)
        half = n_local // 2
        ep_i, dp_i = lax.axis_index('ep'), lax.axis_index('dp')
        own_src = [dp_i * n_ep + i for i in range(n_ep)]
        far_src = [(1 - dp_i) * n_ep + jnp.bitwise_xor(ep_i, i) for i in (0, 2, 1, 3)]
        place = jnp.stack([ep_i * (n_local * cap), dp_i] + own_src + far_src).astype(jnp.int32)
        across = jnp.bitwise_xor(ep_i, 2)

        packed = jnp.concatenate([route_a.astype(F32), route_b.astype(F32), gate_a, gate_b], axis=1)
        plan_row, plan_col = make_plan(packed, cap)
        plans = lax.all_gather(plan_row, ('dp', 'ep'))

        def give_back(rows):
            returned = lax.all_to_all(rows, 'ep', 0, 0)
            return returned.reshape((-1,) + rows.shape[3:])

        def near(tokens):
            return lax.all_gather(tokens, 'ep')

        def cross(tokens, gathered):
            next_chip = lax.dynamic_index_in_dim(gathered, across, 0, False)
            return [lax.ppermute(t, 'dp', swap_dp) for t in (tokens, next_chip)]

        def far(crossed, after):
            crossed, _ = hold((tuple(crossed), after))
            return crossed + tuple(lax.ppermute(t, 'ep', swap_core) for t in crossed)

        def pick(tokens, layer, with_gate=False):
            return pick_rows(tokens, plans, place, layer, n_local, cap, with_gate)

        weights_a, weights_b = (w1_a, w3_a, w2_a), (w1_b, w3_b, w2_b)

        rows_a = pick(near(x_start), 0)
        out_a = [ffn(rows_a, *weights_a, i * half, half) for i in range(2)]
        back_a, out_a[1] = hold((give_back(out_a[0]), out_a[1]))
        x_mid = combine(mix_kernel, 0, x_start, plan_col, [back_a, give_back(out_a[1])], n_ep)

        x_kept, grad_kept, x_mid = hold((x_start, grad_out, x_mid))
        near_x = near(x_mid)
        far_x = cross(x_mid, near_x)
        rows_b = pick(near_x, 1)
        out_b = ffn(rows_b, *weights_b, 0, n_local)

        near_dy, out_b = hold((near(grad_kept), out_b))
        far_dy = cross(grad_kept, near_dy)
        dy_b, gates_b = pick(near_dy, 1, True)
        own_b = [act(rows_b, dy_b, gates_b, *weights_b, 0, half, True)]
        own_b.append(act(rows_b, dy_b, gates_b, *weights_b, half, n_local - half, True,
                           tuple(own_b[0][:3])))
        back_du, own_b[1] = hold((give_back(own_b[0][3]), tuple(own_b[1])))
        du_b = [back_du, give_back(own_b[1][3])]
        dgate_b = give_back(jnp.concatenate([o[4][..., 0] for o in own_b], axis=1))
        near_a = near(x_kept)
        far_a = cross(x_kept, near_a)
        rows_a2 = pick(near_a, 0)
        rows_b_far = pick(far(far_x, own_b[0][0]), 1)
        dy_b_far, gates_b_far = pick(far(far_dy, own_b[1][0]), 1, True)
        du_b[1], dgate_b, rows_a2, rows_b_far, dy_b_far = hold((du_b[1], dgate_b, rows_a2, rows_b_far, dy_b_far))
        grad_mid = combine(add_kernel, 1, grad_kept, plan_col, du_b, n_ep)
        dgate_b = gate_back(1, plan_col, dgate_b.reshape(1, -1))

        near_dx = near(grad_mid)
        other_b = act(rows_b_far, dy_b_far, gates_b_far, *weights_b, 0, n_local, False)
        near_dx, other_b, out_b = hold((near_dx, tuple(other_b), out_b))
        far_dx = cross(grad_mid, near_dx)
        dy_a, gates_a = pick(near_dx, 0, True)
        own_a = act(rows_a2, dy_a, gates_a, *weights_a, 0, n_local, True)
        back_b = give_back(out_b)
        own_a, back_b, other_b = hold((tuple(own_a), back_b, other_b))
        du_a = give_back(own_a[3])
        dgate_a = give_back(own_a[4][..., 0])
        x_final = combine(mix_kernel, 1, x_mid, plan_col, [back_b], n_ep)
        dws_b = dweights((rows_b, dy_b, gates_b) + tuple(own_b[1][:3]), (rows_b_far, dy_b_far, gates_b_far) + tuple(other_b),
                         place, n_dp)
        rows_a_far = pick(far(far_a, own_a[0]), 0)
        dy_a_far, gates_a_far = pick(far(far_dx, own_a[0]), 0, True)
        other_a = act(rows_a_far, dy_a_far, gates_a_far, *weights_a, 0, n_local, False)
        dws_a = dweights((rows_a2, dy_a, gates_a) + tuple(own_a[:3]), (rows_a_far, dy_a_far, gates_a_far) + tuple(other_a),
                         place, n_dp)
        du_a, dws_a, dws_b, x_final = hold((du_a, tuple(dws_a), tuple(dws_b), x_final))
        grad_x = combine(add_kernel, 0, grad_mid, plan_col, [du_a], n_ep)
        dgate_a = gate_back(0, plan_col, dgate_a.reshape(1, -1))
        return (x_final, grad_x) + tuple(dws_a) + tuple(dws_b) + (dgate_a, dgate_b)

    return jax.shard_map(local_step, mesh=mesh,
                         in_specs=(tok_spec,) * 6 + (weight_spec,) * 6,
                         out_specs=(tok_spec, tok_spec) + (grad_spec,) * 6 + (tok_spec, tok_spec),
                         check_vma=False)
```
